256 devices in a mesh: grp: 4 (over x), wide: 64 (over y, z, core).
Axes of the slice: x: 4, y: 4, z: 8, core: 2. Of those that a mesh axis runs over, the one named last changes fastest.
Arguments:
- leaf_entries: float32 [4, 128, 512, 512], P('grp', 'wide'), may hold values from -8 to 14, as said below
- leaf_tiles: int32 [4, 128], P('grp', 'wide'), may hold values from 1 to 3
- leaf_map: int32 [4, 128, 3], P('grp', 'wide'), may hold values from 0 to 7, as said below
- mid_entries: float32 [4, 64, 1024, 1024], P('grp', 'wide'), may hold values from -8 to 14, as said below
- mid_tiles: int32 [4, 64], P('grp', 'wide'), may hold values from 3 to 7, as said below
- mid_map: int32 [4, 64, 7], P('grp', 'wide'), may hold values from 0 to 55, as said below
- root_panel_entries: float32 [4, 7680, 512], P('grp', 'wide'), may hold values from -8 to 14, as said below
- root_update_entries: float32 [4, 64, 896, 896], P('grp', 'wide'), may hold values from -1 to 5, as said below
Outputs:
- root_panel: float32 [4, 7680, 512], P('grp', 'wide')
- top_update: float32 [64, 896, 896], P('wide', 'grp')
The draws below stay inside these ranges and needn't reach their ends.
Inputs may be any that keep to these rules, and one draw needn't show every extreme that they name: `mid_tiles`: each group has a middle front with 7 live update tiles. `leaf_map`: the 3 entries of one leaf are distinct and less than 1 + mid_tiles of its middle front. `mid_map`: entry a of a middle front lies in the block (s + a) mod 8 of 7 consecutive tiles, s a multiple of 1 chosen for each front; so the live tiles of one middle update that land in one block of step four number at most 1, and in every draw some middle update sends exactly 1 to one block. `leaf_entries`: each leaf front is symmetric positive definite. `mid_entries`: each middle front is symmetric positive definite. `root_panel_entries`: the first 512 rows form a symmetric positive definite block. `root_update_entries`: the assembled square of step four before the additions is symmetric.
All inputs are finite; a program needn't handle non-finite values.
Results may differ from the reference program's by a relative error of at most 0.0003.
Values sent between devices are 32-bit elements; how exact they have to be, the bound alone decides.
A program may use at most 128 MiB of HBM per device.

```python
import jax
import jax.numpy as jnp
from jax import lax

TILE = 128
LEAF_DEV = 2
UL = 3
FL = 4
UM = 7
FM = 8
K = 4
UT = 56
R = 60
LEAVES = 128
PCOL = 8
UR = 7
UC = 7
N_GRP = 4
N_WIDE = 64


def unit_matrix(key, order_rows):
    noise = jax.random.normal(key, (order_rows, order_rows), jnp.float32)
    symmetric = (noise + noise.T) * (0.3 / jnp.sqrt(2.0 * order_rows))
    return jnp.eye(order_rows, dtype=jnp.float32) + symmetric


def row_scales(key, order_rows):
    return jnp.exp(jax.random.uniform(key, (order_rows,), jnp.float32, -0.6931472, 0.6931472))


def spread_matrix(key, order_rows, block_rows):
    width = block_rows * 5 // 4
    groups = order_rows // block_rows
    total_cols = groups * width
    noise = jax.random.truncated_normal(key, -3.0, 3.0, (order_rows, total_cols), jnp.float32)
    row_group = jnp.arange(order_rows, dtype=jnp.int32) // block_rows
    column_group = jnp.arange(total_cols, dtype=jnp.int32) // width
    weight_mask = jnp.where(row_group[:, None] == column_group[None, :], 1.0, 0.1)
    factor_rows = noise * weight_mask / jnp.sqrt(jnp.float32(width))
    product = jnp.dot(factor_rows, factor_rows.T, precision=lax.Precision.HIGHEST)
    return 0.5 * (product + product.T) + 0.02 * jnp.eye(order_rows, dtype=jnp.float32)


def dominant_matrix(key, order_rows):
    weight_key, scale_key = jax.random.split(key)
    inner = unit_matrix(weight_key, order_rows)
    root_scale = jnp.sqrt(row_scales(scale_key, order_rows))
    return inner * root_scale[:, None] * root_scale[None, :]


def coupled_front(key, order_rows):
    pivot_key, couple_key, trail_key, scale_key = jax.random.split(key, 4)
    rest_rows = order_rows - TILE
    pivot_block = spread_matrix(pivot_key, TILE, TILE)
    trail_block = unit_matrix(trail_key, rest_rows)
    spread = 0.5 * TILE ** (-0.5)
    coupling = jax.random.normal(couple_key, (rest_rows, TILE), jnp.float32) * spread
    pivot_factor = jnp.linalg.cholesky(pivot_block)
    lower_left = jnp.dot(coupling, pivot_factor.T, precision=lax.Precision.HIGHEST)
    product = jnp.dot(coupling, coupling.T, precision=lax.Precision.HIGHEST)
    lower_right = trail_block + 0.5 * (product + product.T)
    upper_half = jnp.concatenate([pivot_block, lower_left.T], axis=1)
    lower_half = jnp.concatenate([lower_left, lower_right], axis=1)
    whole_matrix = jnp.concatenate([upper_half, lower_half], axis=0)
    root_scale = jnp.sqrt(row_scales(scale_key, order_rows))
    return whole_matrix * root_scale[:, None] * root_scale[None, :]


def coupled_batch(key, count, order_rows):

    def draw_single(index):
        return coupled_front(jax.random.fold_in(key, index), order_rows)
    return lax.map(draw_single, jnp.arange(count, dtype=jnp.int32))


def draw_leaf_entries(key, part):
    batch = coupled_batch(jax.random.fold_in(key, 101), N_GRP * LEAVES, FL * TILE)
    return batch.reshape(N_GRP, LEAVES, FL * TILE, FL * TILE)


def draw_mid_entries(key, part):
    batch = coupled_batch(jax.random.fold_in(key, 102), N_GRP * N_WIDE, FM * TILE)
    return batch.reshape(N_GRP, N_WIDE, FM * TILE, FM * TILE)


def middle_live(key):
    live_count = jax.random.randint(jax.random.fold_in(key, 201), (N_GRP, N_WIDE), UL, UM + 1, dtype=jnp.int32)
    chosen = jax.random.randint(jax.random.fold_in(key, 202), (N_GRP, 1), 0, N_WIDE, dtype=jnp.int32)
    filled = jnp.arange(N_WIDE, dtype=jnp.int32)[None, :] == chosen
    return jnp.where(filled, UM, live_count).astype(jnp.int32)


def draw_mid_tiles(key, part):
    return middle_live(key)


def draw_leaf_map(key, part):
    live_count = middle_live(key)
    parent_live = jnp.repeat(live_count, LEAF_DEV, axis=1)
    scores = jax.random.randint(jax.random.fold_in(key, 203), (N_GRP, LEAVES, FM), 0, 1 << 20, dtype=jnp.int32)
    positions = jnp.arange(FM, dtype=jnp.int32)
    scores = scores * FM + positions[None, None, :]
    scores = scores + jnp.where(positions[None, None, :] >= 1 + parent_live[:, :, None], 1 << 26, 0)
    ranking = jnp.argsort(scores, axis=-1, stable=True)
    return ranking[:, :, :UL].astype(jnp.int32)


def draw_mid_map(key, part):
    group_width = 8 // PCOL
    starts = jax.random.randint(jax.random.fold_in(key, 301), (N_GRP, N_WIDE, 1), 0, 8 // group_width, dtype=jnp.int32) * group_width
    block_ids = (starts + jnp.arange(UM, dtype=jnp.int32)[None, None, :]) % 8
    offsets = jax.random.randint(jax.random.fold_in(key, 302), (N_GRP, N_WIDE, UM), 0, UR, dtype=jnp.int32)
    return (block_ids * UR + offsets).astype(jnp.int32)


def draw_root_panel_entries(key, part):

    def draw_group(index):
        group_key = jax.random.fold_in(jax.random.fold_in(key, 401), index)
        pivot_key = jax.random.fold_in(group_key, 0)
        couple_key = jax.random.fold_in(group_key, 1)
        pivot_scale_key = jax.random.fold_in(group_key, 3)
        pivot_inner = spread_matrix(pivot_key, K * TILE, TILE)
        pivot_scale = jnp.sqrt(row_scales(pivot_scale_key, K * TILE))
        pivot_block = pivot_inner * pivot_scale[:, None] * pivot_scale[None, :]
        coupling = jax.random.normal(couple_key, (UT * TILE, K * TILE), jnp.float32) * 0.02
        return jnp.concatenate([pivot_block, coupling], axis=0)
    return lax.map(draw_group, jnp.arange(N_GRP, dtype=jnp.int32))


def draw_root_update_entries(key, part):

    def draw_group(index):
        whole_matrix = dominant_matrix(jax.random.fold_in(jax.random.fold_in(key, 501), index), UT * TILE)
        block_view = whole_matrix.reshape(8, UR * TILE, PCOL, UC * TILE).transpose(0, 2, 1, 3)
        return block_view.reshape(N_WIDE, UR * TILE, UC * TILE)
    return lax.map(draw_group, jnp.arange(N_GRP, dtype=jnp.int32))


def touch_ends(values, rng, low, top_value):
    index_at = [jax.random.randint(jax.random.fold_in(rng, axis), (), 0, length) for axis, length in enumerate(values.shape)]
    widest = values.shape.index(max(values.shape))
    neighbour = index_at[:widest] + [(index_at[widest] + 1) % values.shape[widest]] + index_at[widest + 1:]
    return values.at[tuple(index_at)].set(low).at[tuple(neighbour)].set(top_value)


def setup_inputs(seed: int = 0) -> dict:
    keys = jax.random.split(jax.random.key(seed), 9)
    leaf_entries = draw_leaf_entries(jax.random.fold_in(keys[8], 71), 0)
    leaf_tiles = touch_ends(jax.random.randint(keys[1], (N_GRP, LEAVES), 1, UL + 1), jax.random.fold_in(keys[1], 1), 1, UL).astype(jnp.int32)
    leaf_map = draw_leaf_map(jax.random.fold_in(keys[8], 71), 0)
    mid_entries = draw_mid_entries(jax.random.fold_in(keys[8], 71), 0)
    mid_tiles = draw_mid_tiles(jax.random.fold_in(keys[8], 71), 0)
    mid_map = draw_mid_map(jax.random.fold_in(keys[8], 71), 0)
    root_panel_entries = draw_root_panel_entries(jax.random.fold_in(keys[8], 71), 0)
    root_update_entries = draw_root_update_entries(jax.random.fold_in(keys[8], 71), 0)
    return dict(leaf_entries=leaf_entries, leaf_tiles=leaf_tiles, leaf_map=leaf_map, mid_entries=mid_entries, mid_tiles=mid_tiles, mid_map=mid_map, root_panel_entries=root_panel_entries, root_update_entries=root_update_entries)


def partial_factor(front_mat, live_tiles):
    order_rows = front_mat.shape[0]
    tile_index = jnp.arange(order_rows, dtype=jnp.int32) // TILE
    live_rows = (tile_index < 1 + live_tiles).astype(jnp.float32)
    masked = front_mat * live_rows[:, None] * live_rows[None, :]
    pivot_factor = jnp.linalg.cholesky(masked[:TILE, :TILE])
    coupling = jax.scipy.linalg.solve_triangular(pivot_factor, masked[TILE:, :TILE].T, lower=True).T
    product = jnp.dot(coupling.astype(jnp.float32), coupling.T.astype(jnp.float32), precision=lax.Precision.HIGHEST, preferred_element_type=jnp.float32)
    return masked[TILE:, TILE:] - product

def middle_update(leaf_fronts, leaf_live, leaf_maps, middle_front, middle_count):
    leaf_updates = jax.vmap(partial_factor)(leaf_fronts, leaf_live)
    leaf_count = leaf_updates.shape[0]
    leaf_blocks = leaf_updates.reshape(leaf_count, UL, TILE, UL, TILE)
    onehot = (leaf_maps[:, None, :] == jnp.arange(FM, dtype=jnp.int32)[None, :, None]).astype(jnp.float32)
    spread = jnp.einsum('lpa,laxby->lpxby', onehot, leaf_blocks, precision=lax.Precision.HIGHEST)
    added = jnp.einsum('lpxby,lqb->pxqy', spread, onehot, precision=lax.Precision.HIGHEST)
    assembled = middle_front + added.reshape(FM * TILE, FM * TILE)
    return partial_factor(assembled, middle_count)

def reference(leaf_entries, leaf_tiles, leaf_map, mid_entries, mid_tiles, mid_map, root_panel_entries, root_update_entries):
    grid_cols = N_WIDE // 8
    row_tiles = UT // 8
    column_tiles = UT // grid_cols
    panels = []
    total = jnp.zeros((UT, UT, TILE, TILE), jnp.float32)
    all_tile = jnp.arange(R * TILE, dtype=jnp.int32) // TILE
    for group in range(N_GRP):
        leaf_fronts = leaf_entries[group].reshape(N_WIDE, LEAF_DEV, FL * TILE, FL * TILE)
        leaf_live = leaf_tiles[group].reshape(N_WIDE, LEAF_DEV)
        leaf_maps = leaf_map[group].reshape(N_WIDE, LEAF_DEV, UL)

        def one_middle(packed):
            return middle_update(packed[0], packed[1], packed[2], packed[3], packed[4])
        middle_updates = lax.map(one_middle, (leaf_fronts, leaf_live, leaf_maps, mid_entries[group], mid_tiles[group]))
        block_view = root_update_entries[group].reshape(8, grid_cols, row_tiles, TILE, column_tiles, TILE)
        update_tiles = block_view.transpose(0, 2, 1, 4, 3, 5).reshape(UT, UT, TILE, TILE)
        group_map = mid_map[group]

        def add_middle(index, current):
            pieces = middle_updates[index].reshape(UM, TILE, UM, TILE).transpose(0, 2, 1, 3)
            targets = group_map[index]
            return current.at[targets[:, None], targets[None, :]].add(pieces)
        update_tiles = lax.fori_loop(0, N_WIDE, add_middle, update_tiles)
        panel = root_panel_entries[group]
        columns = []
        for pivot in range(K):
            column = panel[:, pivot * TILE:(pivot + 1) * TILE]
            factor = jnp.linalg.cholesky(column[pivot * TILE:(pivot + 1) * TILE])
            solved = jax.scipy.linalg.solve_triangular(factor, column.T, lower=True).T
            solved = jnp.where(all_tile[:, None] > pivot, solved, 0.0)
            solved = solved.at[pivot * TILE:(pivot + 1) * TILE].set(factor)
            leading = jnp.where(all_tile[:K * TILE, None] > pivot, solved[:K * TILE], 0.0)
            panel = panel - jnp.dot(solved.astype(jnp.float32), leading.T.astype(jnp.float32), precision=lax.Precision.HIGHEST, preferred_element_type=jnp.float32)
            lower_rows = solved[K * TILE:].reshape(UT, TILE, TILE)
            update_tiles = update_tiles - jnp.einsum('axk,byk->abxy', lower_rows, lower_rows, precision=lax.Precision.HIGHEST)
            columns.append(solved)
        panels.append(jnp.concatenate(columns, axis=1))
        total = total + update_tiles
    top_view = total.reshape(8, row_tiles, grid_cols, column_tiles, TILE, TILE).transpose(0, 2, 1, 4, 3, 5)
    top_update = top_view.reshape(N_WIDE, row_tiles * TILE, column_tiles * TILE)
    return (jnp.stack(panels), top_update)
```

```python
import functools

import jax
import jax.numpy as jnp
from jax import lax
from jax.experimental import pallas as pl
from jax.experimental.pallas import tpu as pltpu
from jax.sharding import PartitionSpec as P

TILE = 128
UL = 3
UM = 7
K = 4
UR = 7
UC = 7
BLOCK = UR * TILE
PIVOT = K * TILE
SLOT = TILE + 8
MESH = pl.DeviceIdType.MESH
HIGHEST = lax.Precision.HIGHEST
NN = ((1,), (0,))
NT = ((1,), (1,))
TN = ((0,), (0,))
VMEM_BYTES = 60 * 1024 * 1024


def dot_exact(a, b, dims=NN):
    return lax.dot_general(
        a, b, (dims, ((), ())), precision=HIGHEST, preferred_element_type=jnp.float32
    )


def split_high_low(a):
    high = a.astype(jnp.bfloat16)
    low = (a - high.astype(jnp.float32)).astype(jnp.bfloat16)
    return high, low


def dot_split(a, b):
    a_high, a_low = split_high_low(a)
    b_high, b_low = split_high_low(b)
    left = jnp.concatenate([a_high, a_high, a_low], axis=1)
    right = jnp.concatenate([b_high, b_low, b_high], axis=1)
    return lax.dot_general(left, right, (NT, ((), ())), preferred_element_type=jnp.float32)


def base_factor(mats, n):
    count = n // 8
    number = range(len(mats))
    rest = [[m[8 * i : 8 * i + 8, :] for i in range(count)] for m in mats]
    row = lax.broadcasted_iota(jnp.int32, (8, n), 0)
    col = lax.broadcasted_iota(jnp.int32, (8, n), 1)
    unit = [[(row + 8 * i == col).astype(jnp.float32) for i in range(count)] for _ in mats]
    upper = [[None] * count for _ in mats]
    inverse = [[None] * count for _ in mats]

    def spread(v, j):
        return jnp.broadcast_to(v[j : j + 1, :], (8, n))

    for kb in range(count):
        cols = [
            [
                [
                    jnp.broadcast_to(rest[p][i][:, 8 * kb + j : 8 * kb + j + 1], (8, n))
                    for i in range(kb, count)
                ]
                for j in range(8)
            ]
            for p in number
        ]
        top = [rest[p][kb] for p in number]
        top_unit = [unit[p][kb] for p in number]
        us = [[] for _ in mats]
        xs = [[] for _ in mats]
        for j in range(8):
            for p in number:
                scale = lax.rsqrt(spread(cols[p][j][0], j))
                cols[p][j] = [c * scale for c in cols[p][j]]
                us[p].append(spread(top[p], j) * scale)
                xs[p].append(spread(top_unit[p], j) * scale)
                if j < 7:
                    top[p] = top[p] - cols[p][j][0] * us[p][j]
                    top_unit[p] = top_unit[p] - cols[p][j][0] * xs[p][j]
                for later in range(j + 1, 8):
                    factor = spread(cols[p][j][0], later)
                    cols[p][later] = [c - d * factor for c, d in zip(cols[p][later], cols[p][j])]
        for p in number:
            u, x = us[p][0], xs[p][0]
            for j in range(1, 8):
                u = jnp.where(row == j, us[p][j], u)
                x = jnp.where(row == j, xs[p][j], x)
            upper[p][kb] = jnp.where(col >= row + 8 * kb, u, 0.0)
            inverse[p][kb] = x
            for i in range(kb + 1, count):
                a, b = rest[p][i], unit[p][i]
                for j in range(8):
                    a = a - cols[p][j][i - kb] * us[p][j]
                    b = b - cols[p][j][i - kb] * xs[p][j]
                rest[p][i], unit[p][i] = a, b
    return [jnp.concatenate(u, 0) for u in upper], [jnp.concatenate(x, 0) for x in inverse]


def factor_all(mats, n=TILE):
    if n == 32:
        return base_factor(mats, n)
    h = n // 2
    u1, x1 = factor_all([m[:h, :h] for m in mats], h)
    u12 = [dot_exact(x, m[:h, h:]) for x, m in zip(x1, mats)]
    below = [m[h:, h:] - dot_exact(u, u, TN) for m, u in zip(mats, u12)]
    u2, x2 = factor_all(below, h)
    mixed = [dot_exact(u, x, TN) for u, x in zip(u12, x1)]
    x21 = [-dot_exact(x, t) for x, t in zip(x2, mixed)]
    zero = jnp.zeros((h, h), jnp.float32)

    def stack(a, b, c, d):
        return jnp.concatenate(
            [jnp.concatenate([a, b], axis=1), jnp.concatenate([c, d], axis=1)], axis=0
        )

    upper = [stack(a, b, zero, d) for a, b, d in zip(u1, u12, u2)]
    inverse = [stack(a, zero, c, d) for a, c, d in zip(x1, x21, x2)]
    return upper, inverse


def fronts_kernel(
    leaf_tiles, leaf_map, mid_tiles, mid_map, leaf_ref, mid_ref, slot_ref, whole_ref, couple_ref
):
    whole_ref[...] = mid_ref[...]
    slot_ref[...] = jnp.zeros_like(slot_ref)
    leaves = leaf_ref.shape[0]
    _, inverse = factor_all([leaf_ref[i, :TILE, :TILE] for i in range(leaves)])
    for i in range(leaves):
        live = leaf_tiles[i]
        coupling = dot_exact(leaf_ref[i, TILE:, :TILE], inverse[i], NT)
        update = leaf_ref[i, TILE:, TILE:] - dot_split(coupling, coupling)
        for a in range(UL):
            for b in range(UL):

                @pl.when((a < live) & (b < live))
                def _():
                    rows = pl.ds(pl.multiple_of(leaf_map[i * UL + a] * TILE, TILE), TILE)
                    columns = pl.ds(pl.multiple_of(leaf_map[i * UL + b] * TILE, TILE), TILE)
                    whole_ref[rows, columns] += update[
                        a * TILE : (a + 1) * TILE, b * TILE : (b + 1) * TILE
                    ]

    _, inverse = factor_all([whole_ref[:TILE, :TILE]])
    couple_ref[...] = dot_exact(whole_ref[TILE:, :TILE], inverse[0], NT)
    live = mid_tiles[0]
    column_spots = lax.broadcasted_iota(jnp.int32, (8, TILE), 1)
    for a in range(UM):
        rows = pl.ds(a * TILE, TILE)
        product = dot_split(couple_ref[rows, :], couple_ref[...])
        update = whole_ref[pl.ds((a + 1) * TILE, TILE), TILE:] - product
        target_row = mid_map[a]
        for b in range(UM):

            @pl.when((a < live) & (b < live))
            def _():
                target_column = mid_map[b]
                row_block, column_block = target_row // UR, target_column // UC
                slot = row_block * 8 + column_block
                slot_ref[slot, :TILE, :] = update[:, b * TILE : (b + 1) * TILE]
                spot = (target_row - row_block * UR) * UC + (target_column - column_block * UC)
                slot_ref[slot, TILE:, :] = jnp.broadcast_to(
                    (spot + 1).astype(jnp.float32), (8, TILE)
                )


def solve_rows(rows, lower, inverse):
    solved = []
    for k in range(K):
        part = rows[:, k * TILE : (k + 1) * TILE]
        for j in range(k):
            part = part - dot_split(solved[j], lower[k][j])
        solved.append(dot_split(part, inverse[k]))
    return solved


def root_kernel(position, pivot_ref, row_ref, column_ref, own_ref, entry_ref, panel_ref, block_ref, lower_ref, left_ref, right_ref):
    tile = lambda i, j: pivot_ref[i * TILE : (i + 1) * TILE, j * TILE : (j + 1) * TILE]
    rest = {(i, j): tile(i, j) for i in range(K) for j in range(i + 1)}
    lower = [[None] * K for _ in range(K)]
    inverse = []
    lower_ref[...] = jnp.zeros_like(lower_ref)
    for k in range(K):
        u, x = factor_all([rest[k, k]])
        inverse.append(x[0])
        lower[k][k] = u[0].T
        for i in range(k + 1, K):
            lower[i][k] = dot_exact(rest[i, k], x[0], NT)
        for i in range(k + 1, K):
            for j in range(k + 1, i + 1):
                rest[i, j] = rest[i, j] - dot_exact(lower[i][k], lower[j][k], NT)
        for i in range(k, K):
            lower_ref[i * TILE : (i + 1) * TILE, k * TILE : (k + 1) * TILE] = lower[i][k]
        columns = slice(k * TILE, (k + 1) * TILE)
        for source, target in ((row_ref, left_ref), (column_ref, right_ref)):
            part = source[:, columns]
            for j in range(k):
                part = part - dot_split(target[:, j * TILE : (j + 1) * TILE], lower[k][j])
            target[:, columns] = dot_split(part, x[0])
    own = jnp.concatenate(solve_rows(own_ref[...], lower, inverse), axis=1)
    rows_here = own_ref.shape[0]
    first = position[0] * rows_here
    start = pl.multiple_of(jnp.minimum(first, PIVOT), 8)
    index = first + lax.broadcasted_iota(jnp.int32, own.shape, 0)
    panel_ref[...] = jnp.where(index < PIVOT, lower_ref[pl.ds(start, rows_here), :], own)
    for a in range(UR):
        rows = slice(a * TILE, (a + 1) * TILE)
        block_ref[rows, :] = entry_ref[rows, :] - dot_split(left_ref[rows, :], right_ref[...])


def add_kernel(spots, base_ref, tiles_ref, out_ref):
    out_ref[...] = base_ref[...]

    def step(s, carry):
        spot = spots[s] - 1

        @pl.when(spot >= 0)
        def _():
            rows = pl.ds(pl.multiple_of((spot // UC) * TILE, TILE), TILE)
            columns = pl.ds(pl.multiple_of((spot % UC) * TILE, TILE), TILE)
            out_ref[rows, columns] += tiles_ref[s, :TILE, :]

        return carry

    lax.fori_loop(0, tiles_ref.shape[0], step, 0)


def gather_kernel(
    panel_ref,
    row_ref,
    column_ref,
    pivot_ref,
    first_send,
    local_sem,
    row_first,
    column_first,
    pivot_first,
    row_send,
    row_recv,
    column_send,
    column_recv,
    pivot_send,
    pivot_recv,
):
    group = lax.axis_index("grp")
    me = lax.axis_index("wide")
    p, q = me // 8, me % 8
    core = me % 2
    line = me // 16
    depth = (me // 2) % 8
    devices = pivot_ref.shape[0]
    here = panel_ref.shape[0]
    there = row_ref.shape[1]

    def remote(source, target, send, recv, device):
        return pltpu.make_async_remote_copy(
            src_ref=source,
            dst_ref=target,
            send_sem=send,
            recv_sem=recv,
            device_id=(group, device),
            device_id_type=MESH,
        )

    def routes(i):
        chunk = here * me + i
        is_pivot = chunk < devices
        other = jnp.maximum(chunk - devices, 0)
        piece, slot = other // there, other % there
        block, part = piece // 8, piece % 8
        is_panel = jnp.logical_not(is_pivot)
        home = jnp.minimum(chunk, devices - 1)
        return (
            (row_ref.at[part, slot], row_first.at[slot], piece, is_panel),
            (column_ref.at[part, slot], column_first.at[slot], part * 8 + block, is_panel),
            (pivot_ref.at[home], pivot_first.at[0], home, is_pivot),
        )

    def first():
        for i in range(here):
            for which, (target, sem, device, wanted) in enumerate(routes(i)):

                @pl.when(wanted & (device != me))
                def _():
                    remote(panel_ref.at[i], target, first_send.at[which, i], sem, device).start()

                @pl.when(wanted & (device == me))
                def _():
                    pltpu.make_async_copy(panel_ref.at[i], target, local_sem.at[which, i]).start()

    def arrived(target, sem, source):
        @pl.when(source != me)
        def _():
            remote(panel_ref.at[0], target, first_send.at[0, 0], sem, me).wait_recv()

    first()
    for i in range(here):
        for which, (target, sem, device, wanted) in enumerate(routes(i)):

            @pl.when(wanted & (device == me))
            def _():
                pltpu.make_async_copy(panel_ref.at[i], target, local_sem.at[which, i]).wait()

    sends = []

    def push(source, send, recv, device):
        copy = remote(source, source, send, recv, device)
        copy.start()
        sends.append(copy)

    def landed(target, send, recv):
        remote(target, target, send, recv, me).wait_recv()

    arrived(pivot_ref.at[me], pivot_first.at[0], me // here)
    partner = me + 1 - 2 * core
    push(pivot_ref.at[me], pivot_send.at[0], pivot_recv.at[0], partner)
    for slot in range(there):
        arrived(row_ref.at[q, slot], row_first.at[slot], (devices + there * me + slot) // here)
    for step in range(1, 4):
        push(row_ref.at[q], row_send.at[step], row_recv.at[q // 2], p * 8 + (q + 2 * step) % 8)
    push(row_ref.at[q], row_send.at[0], row_recv.at[4 + q // 2], partner)
    turned = q * 8 + p
    for slot in range(there):
        arrived(column_ref.at[p, slot], column_first.at[slot], (devices + there * turned + slot) // here)
    across = p + 1 - 2 * (p % 2)
    push(column_ref.at[p], column_send.at[0], column_recv.at[16], across * 8 + q)
    for step in range(1, 4):
        push(column_ref.at[p], column_send.at[step], column_recv.at[p], ((p + 2 * step) % 8) * 8 + q)
    landed(pivot_ref.at[partner], pivot_send.at[0], pivot_recv.at[0])
    pair = pivot_ref.at[pl.ds(me - core, 2)]
    for step in range(1, 8):
        push(pair, pivot_send.at[step], pivot_recv.at[1 + depth], line * 16 + ((depth + step) % 8) * 2 + core)
    landed(column_ref.at[across], column_send.at[0], column_recv.at[16])
    for step in range(1, 4):
        push(
            column_ref.at[across], column_send.at[3 + step], column_recv.at[8 + across], ((p + 2 * step) % 8) * 8 + q
        )
    for step in range(1, 4):
        source = (q + 8 - 2 * step) % 8
        landed(row_ref.at[source], row_send.at[step], row_recv.at[source // 2])
        push(row_ref.at[source], row_send.at[3 + step], row_recv.at[4 + source // 2], partner)
    for step in range(1, 8):
        source = (depth + 8 - step) % 8
        landed(pivot_ref.at[pl.ds(line * 16 + source * 2, 2)], pivot_send.at[step], pivot_recv.at[1 + source])
    mine = pivot_ref.at[pl.ds(line * 16, 16)]
    for step in range(1, 4):
        push(mine, pivot_send.at[7 + step], pivot_recv.at[9 + line], ((line + step) % 4) * 16 + depth * 2 + core)
    for step in range(4):
        source = (q + 1 - 2 * core + 2 * step) % 8
        landed(row_ref.at[source], row_send.at[0], row_recv.at[4 + source // 2])
    for step in range(1, 4):
        source = (p + 8 - 2 * step) % 8
        landed(column_ref.at[source], column_send.at[step], column_recv.at[source])
        source = (across + 8 - 2 * step) % 8
        landed(column_ref.at[source], column_send.at[3 + step], column_recv.at[8 + source])
    for step in range(1, 4):
        source = (line + 4 - step) % 4
        landed(pivot_ref.at[pl.ds(source * 16, 16)], pivot_send.at[7 + step], pivot_recv.at[9 + source])
    for copy in sends:
        copy.wait_send()
    for i in range(here):
        for which, (target, sem, device, wanted) in enumerate(routes(i)):

            @pl.when(wanted & (device != me))
            def _():
                remote(panel_ref.at[i], target, first_send.at[which, i], sem, device).wait_send()


def vmem():
    return pl.BlockSpec(memory_space=pltpu.VMEM)


def smem():
    return pl.BlockSpec(memory_space=pltpu.SMEM)


def shape(*dims):
    return jax.ShapeDtypeStruct(dims, jnp.float32)


def shards(
    leaf_entries,
    leaf_tiles,
    leaf_map,
    mid_entries,
    mid_tiles,
    mid_map,
    root_panel_entries,
    root_update_entries,
):
    devices = lax.axis_size("wide")
    position = lax.axis_index("wide").astype(jnp.int32).reshape(1)
    panel = root_panel_entries[0]
    rows_here = panel.shape[0]
    width = panel.shape[1]
    chunks = rows_here // 8
    piece = chunks - 1
    row_rows, column_rows, pivot = pl.pallas_call(
        gather_kernel,
        out_shape=[
            shape(8, piece, 8, width),
            shape(8, piece, 8, width),
            shape(devices, 8, width),
        ],
        in_specs=[pl.BlockSpec(memory_space=pl.ANY)],
        out_specs=[vmem()] * 3,
        scratch_shapes=[
            pltpu.SemaphoreType.DMA((3, chunks)),
            pltpu.SemaphoreType.DMA((3, chunks)),
            pltpu.SemaphoreType.DMA((piece,)),
            pltpu.SemaphoreType.DMA((piece,)),
            pltpu.SemaphoreType.DMA((1,)),
            pltpu.SemaphoreType.DMA((7,)),
            pltpu.SemaphoreType.DMA((8,)),
            pltpu.SemaphoreType.DMA((7,)),
            pltpu.SemaphoreType.DMA((17,)),
            pltpu.SemaphoreType.DMA((11,)),
            pltpu.SemaphoreType.DMA((13,)),
        ],
        compiler_params=pltpu.CompilerParams(has_side_effects=True),
        name="gather",
    )(panel.reshape(chunks, 8, width))
    row_rows = row_rows.reshape(BLOCK, width)
    column_rows = column_rows.reshape(BLOCK, width)
    pivot = pivot.reshape(PIVOT, width)
    slots = pl.pallas_call(
        fronts_kernel,
        out_shape=shape(devices, SLOT, TILE),
        in_specs=[smem()] * 4 + [vmem()] * 2,
        out_specs=vmem(),
        scratch_shapes=[
            pltpu.VMEM(mid_entries.shape[2:], jnp.float32),
            pltpu.VMEM((BLOCK, TILE), jnp.float32),
        ],
        compiler_params=pltpu.CompilerParams(vmem_limit_bytes=VMEM_BYTES),
        cost_estimate=pl.CostEstimate(flops=20_000_000_000, bytes_accessed=11_000_000, transcendentals=0),
        name="fronts",
    )(
        leaf_tiles[0],
        leaf_map[0].reshape(-1),
        mid_tiles[0],
        mid_map[0, 0],
        leaf_entries[0],
        mid_entries[0, 0],
    )
    received = lax.all_to_all(slots, "wide", split_axis=0, concat_axis=0, tiled=True)
    root_panel, block = pl.pallas_call(
        root_kernel,
        out_shape=[shape(rows_here, width), shape(BLOCK, BLOCK)],
        in_specs=[smem()] + [vmem()] * 5,
        out_specs=[vmem()] * 2,
        scratch_shapes=[
            pltpu.VMEM((PIVOT + rows_here, PIVOT), jnp.float32),
            pltpu.VMEM((BLOCK, PIVOT), jnp.float32),
            pltpu.VMEM((BLOCK, PIVOT), jnp.float32),
        ],
        compiler_params=pltpu.CompilerParams(vmem_limit_bytes=VMEM_BYTES),
        cost_estimate=pl.CostEstimate(flops=30_000_000_000, bytes_accessed=11_000_000, transcendentals=0),
        name="root",
    )(position, pivot, row_rows, column_rows, panel, root_update_entries[0, 0])
    spots = received[:, TILE, 0].astype(jnp.int32)
    total = pl.pallas_call(
        add_kernel,
        out_shape=shape(BLOCK, BLOCK),
        in_specs=[smem(), vmem(), vmem()],
        out_specs=vmem(),
        compiler_params=pltpu.CompilerParams(vmem_limit_bytes=VMEM_BYTES),
        name="add_tiles",
    )(spots, block, received)
    top_part = lax.psum_scatter(total, "grp", scatter_dimension=0, tiled=True)
    return (root_panel[None], top_part[None])


def solution(mesh):
    placed = (
        P("grp", "wide", None, None),
        P("grp", "wide"),
        P("grp", "wide", None),
        P("grp", "wide", None, None),
        P("grp", "wide"),
        P("grp", "wide", None),
        P("grp", "wide", None),
        P("grp", "wide", None, None),
    )
    return jax.shard_map(
        shards,
        mesh=mesh,
        in_specs=placed,
        out_specs=(P("grp", "wide", None), P("wide", "grp", None)),
        check_vma=False,
    )
```

```python
import functools

import jax
import jax.numpy as jnp
from jax import lax
from jax.experimental import pallas as pl
from jax.experimental.pallas import tpu as pltpu
from jax.sharding import PartitionSpec as P

TILE = 128
UL = 3
UM = 7
K = 4
UR = 7
UC = 7
BLOCK = UR * TILE
PIVOT = K * TILE
SLOT = TILE + 8
GROUPS = 4
CHUNK = BLOCK // GROUPS
MESH = pl.DeviceIdType.MESH
HIGHEST = lax.Precision.HIGHEST
NN = ((1,), (0,))
NT = ((1,), (1,))
TN = ((0,), (0,))
VMEM_BYTES = 60 * 1024 * 1024


def dot_exact(a, b, dims=NN):
    return lax.dot_general(
        a, b, (dims, ((), ())), precision=HIGHEST, preferred_element_type=jnp.float32
    )


def split_high_low(a):
    high = a.astype(jnp.bfloat16)
    low = (a - high.astype(jnp.float32)).astype(jnp.bfloat16)
    return high, low


def dot_split(a, b):
    a_high, a_low = split_high_low(a)
    b_high, b_low = split_high_low(b)
    left = jnp.concatenate([a_high, a_high, a_low], axis=1)
    right = jnp.concatenate([b_high, b_low, b_high], axis=1)
    return lax.dot_general(left, right, (NT, ((), ())), preferred_element_type=jnp.float32)


def base_factor(mats, n):
    count = n // 8
    number = range(len(mats))
    rest = [[m[8 * i : 8 * i + 8, :] for i in range(count)] for m in mats]
    row = lax.broadcasted_iota(jnp.int32, (8, n), 0)
    col = lax.broadcasted_iota(jnp.int32, (8, n), 1)
    unit = [[(row + 8 * i == col).astype(jnp.float32) for i in range(count)] for _ in mats]
    upper = [[None] * count for _ in mats]
    inverse = [[None] * count for _ in mats]

    def spread(v, j):
        return jnp.broadcast_to(v[j : j + 1, :], (8, n))

    for kb in range(count):
        cols = [
            [
                [
                    jnp.broadcast_to(rest[p][i][:, 8 * kb + j : 8 * kb + j + 1], (8, n))
                    for i in range(kb, count)
                ]
                for j in range(8)
            ]
            for p in number
        ]
        top = [rest[p][kb] for p in number]
        top_unit = [unit[p][kb] for p in number]
        us = [[] for _ in mats]
        xs = [[] for _ in mats]
        for j in range(8):
            for p in number:
                scale = lax.rsqrt(spread(cols[p][j][0], j))
                cols[p][j] = [c * scale for c in cols[p][j]]
                us[p].append(spread(top[p], j) * scale)
                xs[p].append(spread(top_unit[p], j) * scale)
                if j < 7:
                    top[p] = top[p] - cols[p][j][0] * us[p][j]
                    top_unit[p] = top_unit[p] - cols[p][j][0] * xs[p][j]
                for later in range(j + 1, 8):
                    factor = spread(cols[p][j][0], later)
                    cols[p][later] = [c - d * factor for c, d in zip(cols[p][later], cols[p][j])]
        for p in number:
            u, x = us[p][0], xs[p][0]
            for j in range(1, 8):
                u = jnp.where(row == j, us[p][j], u)
                x = jnp.where(row == j, xs[p][j], x)
            upper[p][kb] = jnp.where(col >= row + 8 * kb, u, 0.0)
            inverse[p][kb] = x
            for i in range(kb + 1, count):
                a, b = rest[p][i], unit[p][i]
                for j in range(8):
                    a = a - cols[p][j][i - kb] * us[p][j]
                    b = b - cols[p][j][i - kb] * xs[p][j]
                rest[p][i], unit[p][i] = a, b
    return [jnp.concatenate(u, 0) for u in upper], [jnp.concatenate(x, 0) for x in inverse]


def factor_all(mats, n=TILE):
    if n == 32:
        return base_factor(mats, n)
    h = n // 2
    u1, x1 = factor_all([m[:h, :h] for m in mats], h)
    u12 = [dot_exact(x, m[:h, h:]) for x, m in zip(x1, mats)]
    below = [m[h:, h:] - dot_exact(u, u, TN) for m, u in zip(mats, u12)]
    u2, x2 = factor_all(below, h)
    mixed = [dot_exact(u, x, TN) for u, x in zip(u12, x1)]
    x21 = [-dot_exact(x, t) for x, t in zip(x2, mixed)]
    zero = jnp.zeros((h, h), jnp.float32)

    def stack(a, b, c, d):
        return jnp.concatenate(
            [jnp.concatenate([a, b], axis=1), jnp.concatenate([c, d], axis=1)], axis=0
        )

    upper = [stack(a, b, zero, d) for a, b, d in zip(u1, u12, u2)]
    inverse = [stack(a, zero, c, d) for a, c, d in zip(x1, x21, x2)]
    return upper, inverse


def fronts_kernel(
    leaf_tiles,
    leaf_map,
    mid_tiles,
    mid_map,
    leaf_ref,
    mid_ref,
    after_ref,
    slot_ref,
    whole_ref,
    couple_ref,
):
    del after_ref

    whole_ref[...] = mid_ref[...]
    slot_ref[...] = jnp.zeros_like(slot_ref)
    leaves = leaf_ref.shape[0]
    _, inverse = factor_all([leaf_ref[i, :TILE, :TILE] for i in range(leaves)])
    for i in range(leaves):
        live = leaf_tiles[i]
        coupling = dot_exact(leaf_ref[i, TILE:, :TILE], inverse[i], NT)
        update = leaf_ref[i, TILE:, TILE:] - dot_split(coupling, coupling)
        for a in range(UL):
            for b in range(UL):

                @pl.when((a < live) & (b < live))
                def _():
                    rows = pl.ds(pl.multiple_of(leaf_map[i * UL + a] * TILE, TILE), TILE)
                    columns = pl.ds(pl.multiple_of(leaf_map[i * UL + b] * TILE, TILE), TILE)
                    whole_ref[rows, columns] += update[
                        a * TILE : (a + 1) * TILE, b * TILE : (b + 1) * TILE
                    ]

    _, inverse = factor_all([whole_ref[:TILE, :TILE]])
    couple_ref[...] = dot_exact(whole_ref[TILE:, :TILE], inverse[0], NT)
    live = mid_tiles[0]
    column_spots = lax.broadcasted_iota(jnp.int32, (8, TILE), 1)
    for a in range(UM):
        rows = pl.ds(a * TILE, TILE)
        product = dot_split(couple_ref[rows, :], couple_ref[...])
        update = whole_ref[pl.ds((a + 1) * TILE, TILE), TILE:] - product
        target_row = mid_map[a]
        for b in range(UM):

            @pl.when((a < live) & (b < live))
            def _():
                target_column = mid_map[b]
                row_block, column_block = target_row // UR, target_column // UC
                slot = row_block * 8 + column_block
                slot_ref[slot, :TILE, :] = update[:, b * TILE : (b + 1) * TILE]
                spot = (target_row - row_block * UR) * UC + (target_column - column_block * UC)
                slot_ref[slot, TILE:, :] = jnp.broadcast_to(
                    (spot + 1).astype(jnp.float32), (8, TILE)
                )


def solve_rows(rows, lower, inverse):
    solved = []
    for k in range(K):
        part = rows[:, k * TILE : (k + 1) * TILE]
        for j in range(k):
            part = part - dot_split(solved[j], lower[k][j])
        solved.append(dot_split(part, inverse[k]))
    return solved


def root_kernel(position, pivot_ref, row_ref, column_ref, own_ref, entry_ref, panel_ref, block_ref, lower_ref, left_ref, right_ref):
    tile = lambda i, j: pivot_ref[i * TILE : (i + 1) * TILE, j * TILE : (j + 1) * TILE]
    rest = {(i, j): tile(i, j) for i in range(K) for j in range(i + 1)}
    lower = [[None] * K for _ in range(K)]
    inverse = []
    lower_ref[...] = jnp.zeros_like(lower_ref)
    for k in range(K):
        u, x = factor_all([rest[k, k]])
        inverse.append(x[0])
        lower[k][k] = u[0].T
        for i in range(k + 1, K):
            lower[i][k] = dot_exact(rest[i, k], x[0], NT)
        for i in range(k + 1, K):
            for j in range(k + 1, i + 1):
                rest[i, j] = rest[i, j] - dot_exact(lower[i][k], lower[j][k], NT)
        for i in range(k, K):
            lower_ref[i * TILE : (i + 1) * TILE, k * TILE : (k + 1) * TILE] = lower[i][k]
        columns = slice(k * TILE, (k + 1) * TILE)
        for source, target in ((row_ref, left_ref), (column_ref, right_ref)):
            part = source[:, columns]
            for j in range(k):
                part = part - dot_split(target[:, j * TILE : (j + 1) * TILE], lower[k][j])
            target[:, columns] = dot_split(part, x[0])
    own = jnp.concatenate(solve_rows(own_ref[...], lower, inverse), axis=1)
    rows_here = own_ref.shape[0]
    first = position[0] * rows_here
    start = pl.multiple_of(jnp.minimum(first, PIVOT), 8)
    index = first + lax.broadcasted_iota(jnp.int32, own.shape, 0)
    panel_ref[...] = jnp.where(index < PIVOT, lower_ref[pl.ds(start, rows_here), :], own)
    for a in range(UR):
        rows = slice(a * TILE, (a + 1) * TILE)
        block_ref[rows, :] = entry_ref[rows, :] - dot_split(left_ref[rows, :], right_ref[...])


def add_kernel(spots, base_ref, tiles_ref, out_ref):
    out_ref[...] = base_ref[...]

    def step(s, carry):
        spot = spots[s] - 1

        @pl.when(spot >= 0)
        def _():
            rows = pl.ds(pl.multiple_of((spot // UC) * TILE, TILE), TILE)
            columns = pl.ds(pl.multiple_of((spot % UC) * TILE, TILE), TILE)
            out_ref[rows, columns] += tiles_ref[s, :TILE, :]

        return carry

    lax.fori_loop(0, tiles_ref.shape[0], step, 0)


def gather_kernel(
    panel_ref,
    row_ref,
    column_ref,
    pivot_ref,
    first_send,
    local_sem,
    row_first,
    column_first,
    pivot_first,
    row_send,
    row_recv,
    column_send,
    column_recv,
    pivot_send,
    pivot_recv,
):
    group = lax.axis_index("grp")
    me = lax.axis_index("wide")
    p, q = me // 8, me % 8
    core = me % 2
    line = me // 16
    depth = (me // 2) % 8
    devices = pivot_ref.shape[0]
    here = panel_ref.shape[0]
    there = row_ref.shape[1]

    def remote(source, target, send, recv, device):
        return pltpu.make_async_remote_copy(
            src_ref=source,
            dst_ref=target,
            send_sem=send,
            recv_sem=recv,
            device_id=(group, device),
            device_id_type=MESH,
        )

    def routes(i):
        chunk = here * me + i
        is_pivot = chunk < devices
        other = jnp.maximum(chunk - devices, 0)
        piece, slot = other // there, other % there
        block, part = piece // 8, piece % 8
        is_panel = jnp.logical_not(is_pivot)
        home = jnp.minimum(chunk, devices - 1)
        return (
            (column_ref.at[part, slot], column_first.at[slot], part * 8 + block, is_panel),
            (row_ref.at[part, slot], row_first.at[slot], piece, is_panel),
            (pivot_ref.at[home], pivot_first.at[0], home, is_pivot),
        )

    def first():
        for i in range(here):
            for which, (target, sem, device, wanted) in enumerate(routes(i)):

                @pl.when(wanted & (device != me))
                def _():
                    remote(panel_ref.at[i], target, first_send.at[which, i], sem, device).start()

                @pl.when(wanted & (device == me))
                def _():
                    pltpu.make_async_copy(panel_ref.at[i], target, local_sem.at[which, i]).start()

    def arrived(target, sem, source):
        @pl.when(source != me)
        def _():
            remote(panel_ref.at[0], target, first_send.at[0, 0], sem, me).wait_recv()

    barrier = pltpu.get_barrier_semaphore()

    def greet(step, carry):
        pl.semaphore_signal(
            barrier, inc=1, device_id=(group, (me + step) % devices), device_id_type=MESH
        )
        return carry

    lax.fori_loop(1, devices, greet, 0)
    pl.semaphore_wait(barrier, devices - 1)
    first()
    for i in range(here):
        for which, (target, sem, device, wanted) in enumerate(routes(i)):

            @pl.when(wanted & (device == me))
            def _():
                pltpu.make_async_copy(panel_ref.at[i], target, local_sem.at[which, i]).wait()

    sends = []

    def push(source, send, recv, device):
        copy = remote(source, source, send, recv, device)
        copy.start()
        sends.append(copy)

    def landed(target, send, recv):
        remote(target, target, send, recv, me).wait_recv()

    arrived(pivot_ref.at[me], pivot_first.at[0], me // here)
    partner = me + 1 - 2 * core
    push(pivot_ref.at[me], pivot_send.at[0], pivot_recv.at[0], partner)
    turned = q * 8 + p
    for slot in range(there):
        arrived(column_ref.at[p, slot], column_first.at[slot], (devices + there * turned + slot) // here)
    across = p + 1 - 2 * (p % 2)
    push(column_ref.at[p], column_send.at[0], column_recv.at[16], across * 8 + q)
    for step in range(1, 4):
        push(column_ref.at[p], column_send.at[step], column_recv.at[p], ((p + 2 * step) % 8) * 8 + q)
    landed(pivot_ref.at[partner], pivot_send.at[0], pivot_recv.at[0])
    pair = pivot_ref.at[pl.ds(me - core, 2)]
    for step in range(1, 8):
        push(pair, pivot_send.at[step], pivot_recv.at[1 + depth], line * 16 + ((depth + step) % 8) * 2 + core)
    for slot in range(there):
        arrived(row_ref.at[q, slot], row_first.at[slot], (devices + there * me + slot) // here)
    for step in range(1, 4):
        push(row_ref.at[q], row_send.at[step], row_recv.at[q // 2], p * 8 + (q + 2 * step) % 8)
    push(row_ref.at[q], row_send.at[0], row_recv.at[4 + q // 2], partner)
    landed(column_ref.at[across], column_send.at[0], column_recv.at[16])
    for step in range(1, 4):
        push(
            column_ref.at[across], column_send.at[3 + step], column_recv.at[8 + across], ((p + 2 * step) % 8) * 8 + q
        )
    for step in range(1, 4):
        source = (q + 8 - 2 * step) % 8
        landed(row_ref.at[source], row_send.at[step], row_recv.at[source // 2])
        push(row_ref.at[source], row_send.at[3 + step], row_recv.at[4 + source // 2], partner)
    for step in range(1, 8):
        source = (depth + 8 - step) % 8
        landed(pivot_ref.at[pl.ds(line * 16 + source * 2, 2)], pivot_send.at[step], pivot_recv.at[1 + source])
    mine = pivot_ref.at[pl.ds(line * 16, 16)]
    for step in range(1, 4):
        push(mine, pivot_send.at[7 + step], pivot_recv.at[9 + line], ((line + step) % 4) * 16 + depth * 2 + core)
    for step in range(4):
        source = (q + 1 - 2 * core + 2 * step) % 8
        landed(row_ref.at[source], row_send.at[0], row_recv.at[4 + source // 2])
    for step in range(1, 4):
        source = (p + 8 - 2 * step) % 8
        landed(column_ref.at[source], column_send.at[step], column_recv.at[source])
        source = (across + 8 - 2 * step) % 8
        landed(column_ref.at[source], column_send.at[3 + step], column_recv.at[8 + source])
    for step in range(1, 4):
        source = (line + 4 - step) % 4
        landed(pivot_ref.at[pl.ds(source * 16, 16)], pivot_send.at[7 + step], pivot_recv.at[9 + source])
    for copy in sends:
        copy.wait_send()
    for i in range(here):
        for which, (target, sem, device, wanted) in enumerate(routes(i)):

            @pl.when(wanted & (device != me))
            def _():
                remote(panel_ref.at[i], target, first_send.at[which, i], sem, device).wait_send()


def scatter_kernel(total_ref, part_ref, send_sem, recv_sem):
    group = lax.axis_index("grp")
    me = lax.axis_index("wide")
    barrier = pltpu.get_barrier_semaphore()
    for step in range(1, GROUPS):
        pl.semaphore_signal(
            barrier, inc=1, device_id=((group + step) % GROUPS, me), device_id_type=MESH
        )
    stay = pltpu.make_async_copy(
        total_ref.at[pl.ds(group * CHUNK, CHUNK)], part_ref.at[group], send_sem.at[0]
    )
    stay.start()
    pl.semaphore_wait(barrier, GROUPS - 1)

    def send(step):
        x = (group + step) % GROUPS
        return pltpu.make_async_remote_copy(
            src_ref=total_ref.at[pl.ds(x * CHUNK, CHUNK)],
            dst_ref=part_ref.at[group],
            send_sem=send_sem.at[step],
            recv_sem=recv_sem.at[group],
            device_id=(x, me),
            device_id_type=MESH,
        )

    for step in range(1, GROUPS):
        send(step).start()
    stay.wait()
    for step in range(1, GROUPS):
        g = (group + step) % GROUPS
        pltpu.make_async_remote_copy(
            src_ref=total_ref.at[pl.ds(0, CHUNK)],
            dst_ref=part_ref.at[g],
            send_sem=send_sem.at[0],
            recv_sem=recv_sem.at[g],
            device_id=(group, me),
            device_id_type=MESH,
        ).wait_recv()
        send(step).wait_send()


def sum_kernel(part_ref, out_ref):
    out_ref[...] = (part_ref[0] + part_ref[1]) + (part_ref[2] + part_ref[3])


def vmem():
    return pl.BlockSpec(memory_space=pltpu.VMEM)


def smem():
    return pl.BlockSpec(memory_space=pltpu.SMEM)


def shape(*dims):
    return jax.ShapeDtypeStruct(dims, jnp.float32)


def shards(
    leaf_entries,
    leaf_tiles,
    leaf_map,
    mid_entries,
    mid_tiles,
    mid_map,
    root_panel_entries,
    root_update_entries,
):
    devices = lax.axis_size("wide")
    position = lax.axis_index("wide").astype(jnp.int32).reshape(1)
    panel = root_panel_entries[0]
    rows_here = panel.shape[0]
    width = panel.shape[1]
    chunks = rows_here // 8
    piece = chunks - 1
    row_rows, column_rows, pivot = pl.pallas_call(
        gather_kernel,
        out_shape=[
            shape(8, piece, 8, width),
            shape(8, piece, 8, width),
            shape(devices, 8, width),
        ],
        in_specs=[pl.BlockSpec(memory_space=pl.ANY)],
        out_specs=[vmem()] * 3,
        scratch_shapes=[
            pltpu.SemaphoreType.DMA((3, chunks)),
            pltpu.SemaphoreType.DMA((3, chunks)),
            pltpu.SemaphoreType.DMA((piece,)),
            pltpu.SemaphoreType.DMA((piece,)),
            pltpu.SemaphoreType.DMA((1,)),
            pltpu.SemaphoreType.DMA((7,)),
            pltpu.SemaphoreType.DMA((8,)),
            pltpu.SemaphoreType.DMA((7,)),
            pltpu.SemaphoreType.DMA((17,)),
            pltpu.SemaphoreType.DMA((11,)),
            pltpu.SemaphoreType.DMA((13,)),
        ],
        compiler_params=pltpu.CompilerParams(collective_id=0, has_side_effects=True),
        name="gather",
    )(panel.reshape(chunks, 8, width))
    row_rows = row_rows.reshape(BLOCK, width)
    column_rows = column_rows.reshape(BLOCK, width)
    pivot = pivot.reshape(PIVOT, width)
    slots = pl.pallas_call(
        fronts_kernel,
        out_shape=shape(devices, SLOT, TILE),
        in_specs=[smem()] * 4 + [vmem()] * 2 + [pl.BlockSpec(memory_space=pl.ANY)],
        out_specs=vmem(),
        scratch_shapes=[
            pltpu.VMEM(mid_entries.shape[2:], jnp.float32),
            pltpu.VMEM((BLOCK, TILE), jnp.float32),
        ],
        compiler_params=pltpu.CompilerParams(vmem_limit_bytes=VMEM_BYTES),
        cost_estimate=pl.CostEstimate(flops=20_000_000_000, bytes_accessed=11_000_000, transcendentals=0),
        name="fronts",
    )(
        leaf_tiles[0],
        leaf_map[0].reshape(-1),
        mid_tiles[0],
        mid_map[0, 0],
        leaf_entries[0],
        mid_entries[0, 0],
        pivot,
    )
    received = lax.all_to_all(slots, "wide", split_axis=0, concat_axis=0, tiled=True)
    root_panel, block = pl.pallas_call(
        root_kernel,
        out_shape=[shape(rows_here, width), shape(BLOCK, BLOCK)],
        in_specs=[smem()] + [vmem()] * 5,
        out_specs=[vmem()] * 2,
        scratch_shapes=[
            pltpu.VMEM((PIVOT + rows_here, PIVOT), jnp.float32),
            pltpu.VMEM((BLOCK, PIVOT), jnp.float32),
            pltpu.VMEM((BLOCK, PIVOT), jnp.float32),
        ],
        compiler_params=pltpu.CompilerParams(vmem_limit_bytes=VMEM_BYTES),
        cost_estimate=pl.CostEstimate(flops=30_000_000_000, bytes_accessed=11_000_000, transcendentals=0),
        name="root",
    )(position, pivot, row_rows, column_rows, panel, root_update_entries[0, 0])
    spots = received[:, TILE, 0].astype(jnp.int32)
    total = pl.pallas_call(
        add_kernel,
        out_shape=shape(BLOCK, BLOCK),
        in_specs=[smem(), vmem(), vmem()],
        out_specs=vmem(),
        compiler_params=pltpu.CompilerParams(vmem_limit_bytes=VMEM_BYTES),
        name="add_tiles",
    )(spots, block, received)
    parts = pl.pallas_call(
        scatter_kernel,
        out_shape=shape(GROUPS, CHUNK, BLOCK),
        in_specs=[vmem()],
        out_specs=pl.BlockSpec(memory_space=pl.ANY),
        scratch_shapes=[pltpu.SemaphoreType.DMA((GROUPS,)), pltpu.SemaphoreType.DMA((GROUPS,))],
        compiler_params=pltpu.CompilerParams(collective_id=1, has_side_effects=True),
        name="scatter",
    )(total)
    top_part = pl.pallas_call(
        sum_kernel,
        out_shape=shape(CHUNK, BLOCK),
        in_specs=[vmem()],
        out_specs=vmem(),
        compiler_params=pltpu.CompilerParams(vmem_limit_bytes=VMEM_BYTES),
        name="sum_groups",
    )(parts)
    return (root_panel[None], top_part[None])


def solution(mesh):
    placed = (
        P("grp", "wide", None, None),
        P("grp", "wide"),
        P("grp", "wide", None),
        P("grp", "wide", None, None),
        P("grp", "wide"),
        P("grp", "wide", None),
        P("grp", "wide", None),
        P("grp", "wide", None, None),
    )
    return jax.shard_map(
        shards,
        mesh=mesh,
        in_specs=placed,
        out_specs=(P("grp", "wide", None), P("wide", "grp", None)),
        check_vma=False,
    )
```

```python
import functools

import jax
import jax.numpy as jnp
from jax import lax
from jax.experimental import pallas as pl
from jax.experimental.pallas import tpu as pltpu
from jax.sharding import PartitionSpec as P

TILE = 128
UL = 3
UM = 7
K = 4
UR = 7
UC = 7
BLOCK = UR * TILE
PIVOT = K * TILE
GROUPS = 4
CHUNK = BLOCK // GROUPS
MESH = pl.DeviceIdType.MESH
HIGHEST = lax.Precision.HIGHEST
NN = ((1,), (0,))
NT = ((1,), (1,))
TN = ((0,), (0,))
VMEM_BYTES = 60 * 1024 * 1024


def dot_exact(a, b, dims=NN):
    return lax.dot_general(
        a, b, (dims, ((), ())), precision=HIGHEST, preferred_element_type=jnp.float32
    )


def split_high_low(a):
    high = a.astype(jnp.bfloat16)
    low = (a - high.astype(jnp.float32)).astype(jnp.bfloat16)
    return high, low


def dot_split(a, b):
    a_high, a_low = split_high_low(a)
    b_high, b_low = split_high_low(b)
    left = jnp.concatenate([a_high, a_high, a_low], axis=1)
    right = jnp.concatenate([b_high, b_low, b_high], axis=1)
    return lax.dot_general(left, right, (NT, ((), ())), preferred_element_type=jnp.float32)


def base_factor(mats, n):
    count = n // 8
    number = range(len(mats))
    rest = [[m[8 * i : 8 * i + 8, :] for i in range(count)] for m in mats]
    row = lax.broadcasted_iota(jnp.int32, (8, n), 0)
    col = lax.broadcasted_iota(jnp.int32, (8, n), 1)
    unit = [[(row + 8 * i == col).astype(jnp.float32) for i in range(count)] for _ in mats]
    upper = [[None] * count for _ in mats]
    inverse = [[None] * count for _ in mats]

    def spread(v, j):
        return jnp.broadcast_to(v[j : j + 1, :], (8, n))

    for kb in range(count):
        cols = [
            [
                [
                    jnp.broadcast_to(rest[p][i][:, 8 * kb + j : 8 * kb + j + 1], (8, n))
                    for i in range(kb, count)
                ]
                for j in range(8)
            ]
            for p in number
        ]
        top = [rest[p][kb] for p in number]
        top_unit = [unit[p][kb] for p in number]
        us = [[] for _ in mats]
        xs = [[] for _ in mats]
        for j in range(8):
            for p in number:
                scale = lax.rsqrt(spread(cols[p][j][0], j))
                cols[p][j] = [c * scale for c in cols[p][j]]
                us[p].append(spread(top[p], j) * scale)
                xs[p].append(spread(top_unit[p], j) * scale)
                if j < 7:
                    top[p] = top[p] - cols[p][j][0] * us[p][j]
                    top_unit[p] = top_unit[p] - cols[p][j][0] * xs[p][j]
                for later in range(j + 1, 8):
                    factor = spread(cols[p][j][0], later)
                    cols[p][later] = [c - d * factor for c, d in zip(cols[p][later], cols[p][j])]
        for p in number:
            u, x = us[p][0], xs[p][0]
            for j in range(1, 8):
                u = jnp.where(row == j, us[p][j], u)
                x = jnp.where(row == j, xs[p][j], x)
            upper[p][kb] = jnp.where(col >= row + 8 * kb, u, 0.0)
            inverse[p][kb] = x
            for i in range(kb + 1, count):
                a, b = rest[p][i], unit[p][i]
                for j in range(8):
                    a = a - cols[p][j][i - kb] * us[p][j]
                    b = b - cols[p][j][i - kb] * xs[p][j]
                rest[p][i], unit[p][i] = a, b
    return [jnp.concatenate(u, 0) for u in upper], [jnp.concatenate(x, 0) for x in inverse]


def factor_all(mats, n=TILE):
    if n == 32:
        return base_factor(mats, n)
    h = n // 2
    u1, x1 = factor_all([m[:h, :h] for m in mats], h)
    u12 = [dot_exact(x, m[:h, h:]) for x, m in zip(x1, mats)]
    below = [m[h:, h:] - dot_exact(u, u, TN) for m, u in zip(mats, u12)]
    u2, x2 = factor_all(below, h)
    mixed = [dot_exact(u, x, TN) for u, x in zip(u12, x1)]
    x21 = [-dot_exact(x, t) for x, t in zip(x2, mixed)]
    zero = jnp.zeros((h, h), jnp.float32)

    def stack(a, b, c, d):
        return jnp.concatenate(
            [jnp.concatenate([a, b], axis=1), jnp.concatenate([c, d], axis=1)], axis=0
        )

    upper = [stack(a, b, zero, d) for a, b, d in zip(u1, u12, u2)]
    inverse = [stack(a, zero, c, d) for a, c, d in zip(x1, x21, x2)]
    return upper, inverse


def fronts_kernel(
    leaf_tiles,
    leaf_map,
    mid_tiles,
    mid_map,
    leaf_ref,
    mid_ref,
    after_ref,
    slot_ref,
    whole_ref,
    couple_ref,
):
    del after_ref

    whole_ref[...] = mid_ref[...]
    slot_ref[...] = jnp.zeros_like(slot_ref)
    leaves = leaf_ref.shape[0]
    _, inverse = factor_all([leaf_ref[i, :TILE, :TILE] for i in range(leaves)])
    for i in range(leaves):
        live = leaf_tiles[i]
        coupling = dot_exact(leaf_ref[i, TILE:, :TILE], inverse[i], NT)
        update = leaf_ref[i, TILE:, TILE:] - dot_split(coupling, coupling)
        for a in range(UL):
            for b in range(UL):

                @pl.when((a < live) & (b < live))
                def _():
                    rows = pl.ds(pl.multiple_of(leaf_map[i * UL + a] * TILE, TILE), TILE)
                    columns = pl.ds(pl.multiple_of(leaf_map[i * UL + b] * TILE, TILE), TILE)
                    whole_ref[rows, columns] += update[
                        a * TILE : (a + 1) * TILE, b * TILE : (b + 1) * TILE
                    ]

    _, inverse = factor_all([whole_ref[:TILE, :TILE]])
    couple_ref[...] = dot_exact(whole_ref[TILE:, :TILE], inverse[0], NT)
    live = mid_tiles[0]
    for a in range(UM):
        rows = pl.ds(a * TILE, TILE)
        product = dot_split(couple_ref[rows, :], couple_ref[...])
        update = whole_ref[pl.ds((a + 1) * TILE, TILE), TILE:] - product
        target_row = mid_map[a]
        for b in range(UM):

            @pl.when((a < live) & (b < live))
            def _():
                target_column = mid_map[b]
                slot = (target_row // UR) * 8 + target_column // UC
                slot_ref[slot] = update[:, b * TILE : (b + 1) * TILE]


def solve_rows(rows, lower, inverse):
    solved = []
    for k in range(K):
        part = rows[:, k * TILE : (k + 1) * TILE]
        for j in range(k):
            part = part - dot_split(solved[j], lower[k][j])
        solved.append(dot_split(part, inverse[k]))
    return solved


def root_kernel(position, pivot_ref, row_ref, column_ref, own_ref, entry_ref, panel_ref, block_ref, lower_ref, left_ref, right_ref):
    tile = lambda i, j: pivot_ref[i * TILE : (i + 1) * TILE, j * TILE : (j + 1) * TILE]
    rest = {(i, j): tile(i, j) for i in range(K) for j in range(i + 1)}
    lower = [[None] * K for _ in range(K)]
    inverse = []
    lower_ref[...] = jnp.zeros_like(lower_ref)
    for k in range(K):
        u, x = factor_all([rest[k, k]])
        inverse.append(x[0])
        lower[k][k] = u[0].T
        for i in range(k + 1, K):
            lower[i][k] = dot_exact(rest[i, k], x[0], NT)
        for i in range(k + 1, K):
            for j in range(k + 1, i + 1):
                rest[i, j] = rest[i, j] - dot_exact(lower[i][k], lower[j][k], NT)
        for i in range(k, K):
            lower_ref[i * TILE : (i + 1) * TILE, k * TILE : (k + 1) * TILE] = lower[i][k]
        columns = slice(k * TILE, (k + 1) * TILE)
        for source, target in ((row_ref, left_ref), (column_ref, right_ref)):
            part = source[:, columns]
            for j in range(k):
                part = part - dot_split(target[:, j * TILE : (j + 1) * TILE], lower[k][j])
            target[:, columns] = dot_split(part, x[0])
    own = jnp.concatenate(solve_rows(own_ref[...], lower, inverse), axis=1)
    rows_here = own_ref.shape[0]
    first = position[0] * rows_here
    start = pl.multiple_of(jnp.minimum(first, PIVOT), 8)
    index = first + lax.broadcasted_iota(jnp.int32, own.shape, 0)
    panel_ref[...] = jnp.where(index < PIVOT, lower_ref[pl.ds(start, rows_here), :], own)
    for a in range(UR):
        rows = slice(a * TILE, (a + 1) * TILE)
        block_ref[rows, :] = entry_ref[rows, :] - dot_split(left_ref[rows, :], right_ref[...])


def add_kernel(spots, base_ref, tiles_ref, out_ref):
    out_ref[...] = base_ref[...]

    def step(s, carry):
        spot = spots[s]

        @pl.when(spot >= 0)
        def _():
            rows = pl.ds(pl.multiple_of((spot // UC) * TILE, TILE), TILE)
            columns = pl.ds(pl.multiple_of((spot % UC) * TILE, TILE), TILE)
            out_ref[rows, columns] += tiles_ref[s]

        return carry

    lax.fori_loop(0, tiles_ref.shape[0], step, 0)


def gather_kernel(
    panel_ref,
    note_ref,
    row_ref,
    column_ref,
    pivot_ref,
    notes_ref,
    first_send,
    local_sem,
    row_first,
    column_first,
    pivot_first,
    row_send,
    row_recv,
    column_send,
    column_recv,
    pivot_send,
    pivot_recv,
    note_send,
    note_recv,
):
    group = lax.axis_index("grp")
    me = lax.axis_index("wide")
    p, q = me // 8, me % 8
    core = me % 2
    line = me // 16
    depth = (me // 2) % 8
    devices = pivot_ref.shape[0]
    here = panel_ref.shape[0]
    there = row_ref.shape[1]

    def remote(source, target, send, recv, device):
        return pltpu.make_async_remote_copy(
            src_ref=source,
            dst_ref=target,
            send_sem=send,
            recv_sem=recv,
            device_id=(group, device),
            device_id_type=MESH,
        )

    def routes(i):
        chunk = here * me + i
        is_pivot = chunk < devices
        other = jnp.maximum(chunk - devices, 0)
        piece, slot = other // there, other % there
        block, part = piece // 8, piece % 8
        is_panel = jnp.logical_not(is_pivot)
        home = jnp.minimum(chunk, devices - 1)
        return (
            (column_ref.at[part, slot], column_first.at[slot], part * 8 + block, is_panel),
            (row_ref.at[part, slot], row_first.at[slot], piece, is_panel),
            (pivot_ref.at[home], pivot_first.at[0], home, is_pivot),
        )

    def first():
        for i in range(here):
            for which, (target, sem, device, wanted) in enumerate(routes(i)):

                @pl.when(wanted & (device != me))
                def _():
                    remote(panel_ref.at[i], target, first_send.at[which, i], sem, device).start()

                @pl.when(wanted & (device == me))
                def _():
                    pltpu.make_async_copy(panel_ref.at[i], target, local_sem.at[which, i]).start()

    def arrived(target, sem, source):
        @pl.when(source != me)
        def _():
            remote(panel_ref.at[0], target, first_send.at[0, 0], sem, me).wait_recv()

    barrier = pltpu.get_barrier_semaphore()

    def greet(step, carry):
        pl.semaphore_signal(
            barrier, inc=1, device_id=(group, (me + step) % devices), device_id_type=MESH
        )
        return carry

    lax.fori_loop(1, devices, greet, 0)
    pl.semaphore_wait(barrier, devices - 1)
    note = pltpu.make_async_copy(note_ref, notes_ref.at[me], note_recv.at[0])
    note.start()
    first()
    note.wait()
    for i in range(here):
        for which, (target, sem, device, wanted) in enumerate(routes(i)):

            @pl.when(wanted & (device == me))
            def _():
                pltpu.make_async_copy(panel_ref.at[i], target, local_sem.at[which, i]).wait()

    sends = []

    def push(source, send, recv, device):
        copy = remote(source, source, send, recv, device)
        copy.start()
        sends.append(copy)

    def landed(target, send, recv):
        remote(target, target, send, recv, me).wait_recv()

    def notes(first_device, count):
        return notes_ref.at[pl.ds(first_device, count)]

    arrived(pivot_ref.at[me], pivot_first.at[0], me // here)
    partner = me + 1 - 2 * core
    push(pivot_ref.at[me], pivot_send.at[0], pivot_recv.at[0], partner)
    push(notes(me, 1), note_send.at[0], note_recv.at[1], partner)
    turned = q * 8 + p
    for slot in range(there):
        arrived(column_ref.at[p, slot], column_first.at[slot], (devices + there * turned + slot) // here)
    across = p + 1 - 2 * (p % 2)
    push(column_ref.at[p], column_send.at[0], column_recv.at[16], across * 8 + q)
    for step in range(1, 4):
        push(column_ref.at[p], column_send.at[step], column_recv.at[p], ((p + 2 * step) % 8) * 8 + q)
    landed(pivot_ref.at[partner], pivot_send.at[0], pivot_recv.at[0])
    landed(notes(partner, 1), note_send.at[0], note_recv.at[1])
    pair = pivot_ref.at[pl.ds(me - core, 2)]
    for step in range(1, 8):
        device = line * 16 + ((depth + step) % 8) * 2 + core
        push(pair, pivot_send.at[step], pivot_recv.at[1 + depth], device)
        push(notes(me - core, 2), note_send.at[step], note_recv.at[2 + depth], device)
    for slot in range(there):
        arrived(row_ref.at[q, slot], row_first.at[slot], (devices + there * me + slot) // here)
    for step in range(1, 4):
        push(row_ref.at[q], row_send.at[step], row_recv.at[q // 2], p * 8 + (q + 2 * step) % 8)
    push(row_ref.at[q], row_send.at[0], row_recv.at[4 + q // 2], partner)
    landed(column_ref.at[across], column_send.at[0], column_recv.at[16])
    for step in range(1, 4):
        push(
            column_ref.at[across], column_send.at[3 + step], column_recv.at[8 + across], ((p + 2 * step) % 8) * 8 + q
        )
    for step in range(1, 4):
        source = (q + 8 - 2 * step) % 8
        landed(row_ref.at[source], row_send.at[step], row_recv.at[source // 2])
        push(row_ref.at[source], row_send.at[3 + step], row_recv.at[4 + source // 2], partner)
    for step in range(1, 8):
        source = (depth + 8 - step) % 8
        device = line * 16 + source * 2
        landed(pivot_ref.at[pl.ds(device, 2)], pivot_send.at[step], pivot_recv.at[1 + source])
        landed(notes(device, 2), note_send.at[step], note_recv.at[2 + source])
    mine = pivot_ref.at[pl.ds(line * 16, 16)]
    for step in range(1, 4):
        device = ((line + step) % 4) * 16 + depth * 2 + core
        push(mine, pivot_send.at[7 + step], pivot_recv.at[9 + line], device)
        push(notes(line * 16, 16), note_send.at[7 + step], note_recv.at[10 + line], device)
    for step in range(4):
        source = (q + 1 - 2 * core + 2 * step) % 8
        landed(row_ref.at[source], row_send.at[0], row_recv.at[4 + source // 2])
    for step in range(1, 4):
        source = (p + 8 - 2 * step) % 8
        landed(column_ref.at[source], column_send.at[step], column_recv.at[source])
        source = (across + 8 - 2 * step) % 8
        landed(column_ref.at[source], column_send.at[3 + step], column_recv.at[8 + source])
    for step in range(1, 4):
        source = (line + 4 - step) % 4
        landed(pivot_ref.at[pl.ds(source * 16, 16)], pivot_send.at[7 + step], pivot_recv.at[9 + source])
        landed(notes(source * 16, 16), note_send.at[7 + step], note_recv.at[10 + source])
    for copy in sends:
        copy.wait_send()
    for i in range(here):
        for which, (target, sem, device, wanted) in enumerate(routes(i)):

            @pl.when(wanted & (device != me))
            def _():
                remote(panel_ref.at[i], target, first_send.at[which, i], sem, device).wait_send()


def scatter_kernel(total_ref, part_ref, send_sem, recv_sem):
    group = lax.axis_index("grp")
    me = lax.axis_index("wide")
    barrier = pltpu.get_barrier_semaphore()
    for step in range(1, GROUPS):
        pl.semaphore_signal(
            barrier, inc=1, device_id=((group + step) % GROUPS, me), device_id_type=MESH
        )
    stay = pltpu.make_async_copy(
        total_ref.at[pl.ds(group * CHUNK, CHUNK)], part_ref.at[group], send_sem.at[0]
    )
    stay.start()
    pl.semaphore_wait(barrier, GROUPS - 1)

    def send(step):
        x = (group + step) % GROUPS
        return pltpu.make_async_remote_copy(
            src_ref=total_ref.at[pl.ds(x * CHUNK, CHUNK)],
            dst_ref=part_ref.at[group],
            send_sem=send_sem.at[step],
            recv_sem=recv_sem.at[group],
            device_id=(x, me),
            device_id_type=MESH,
        )

    for step in range(1, GROUPS):
        send(step).start()
    stay.wait()
    for step in range(1, GROUPS):
        g = (group + step) % GROUPS
        pltpu.make_async_remote_copy(
            src_ref=total_ref.at[pl.ds(0, CHUNK)],
            dst_ref=part_ref.at[g],
            send_sem=send_sem.at[0],
            recv_sem=recv_sem.at[g],
            device_id=(group, me),
            device_id_type=MESH,
        ).wait_recv()
        send(step).wait_send()


def sum_kernel(part_ref, out_ref):
    out_ref[...] = (part_ref[0] + part_ref[1]) + (part_ref[2] + part_ref[3])


def vmem():
    return pl.BlockSpec(memory_space=pltpu.VMEM)


def smem():
    return pl.BlockSpec(memory_space=pltpu.SMEM)


def shape(*dims):
    return jax.ShapeDtypeStruct(dims, jnp.float32)


def shards(
    leaf_entries,
    leaf_tiles,
    leaf_map,
    mid_entries,
    mid_tiles,
    mid_map,
    root_panel_entries,
    root_update_entries,
):
    devices = lax.axis_size("wide")
    position = lax.axis_index("wide").astype(jnp.int32).reshape(1)
    panel = root_panel_entries[0]
    rows_here = panel.shape[0]
    width = panel.shape[1]
    chunks = rows_here // 8
    piece = chunks - 1
    note = jnp.concatenate([mid_map[0, 0], mid_tiles[0]]).astype(jnp.float32)
    note = jnp.broadcast_to(jnp.pad(note, (0, TILE - UM - 1))[None], (8, TILE))
    row_rows, column_rows, pivot, notes = pl.pallas_call(
        gather_kernel,
        out_shape=[
            shape(8, piece, 8, width),
            shape(8, piece, 8, width),
            shape(devices, 8, width),
            shape(devices, 8, TILE),
        ],
        in_specs=[pl.BlockSpec(memory_space=pl.ANY)] * 2,
        out_specs=[vmem()] * 4,
        scratch_shapes=[
            pltpu.SemaphoreType.DMA((3, chunks)),
            pltpu.SemaphoreType.DMA((3, chunks)),
            pltpu.SemaphoreType.DMA((piece,)),
            pltpu.SemaphoreType.DMA((piece,)),
            pltpu.SemaphoreType.DMA((1,)),
            pltpu.SemaphoreType.DMA((7,)),
            pltpu.SemaphoreType.DMA((8,)),
            pltpu.SemaphoreType.DMA((7,)),
            pltpu.SemaphoreType.DMA((17,)),
            pltpu.SemaphoreType.DMA((11,)),
            pltpu.SemaphoreType.DMA((13,)),
            pltpu.SemaphoreType.DMA((11,)),
            pltpu.SemaphoreType.DMA((14,)),
        ],
        compiler_params=pltpu.CompilerParams(collective_id=0, has_side_effects=True),
        name="gather",
    )(panel.reshape(chunks, 8, width), note)
    row_rows = row_rows.reshape(BLOCK, width)
    column_rows = column_rows.reshape(BLOCK, width)
    pivot = pivot.reshape(PIVOT, width)
    slots = pl.pallas_call(
        fronts_kernel,
        out_shape=shape(devices, TILE, TILE),
        in_specs=[smem()] * 4 + [vmem()] * 2 + [pl.BlockSpec(memory_space=pl.ANY)],
        out_specs=vmem(),
        scratch_shapes=[
            pltpu.VMEM(mid_entries.shape[2:], jnp.float32),
            pltpu.VMEM((BLOCK, TILE), jnp.float32),
        ],
        compiler_params=pltpu.CompilerParams(vmem_limit_bytes=VMEM_BYTES),
        cost_estimate=pl.CostEstimate(flops=20_000_000_000, bytes_accessed=11_000_000, transcendentals=0),
        name="fronts",
    )(
        leaf_tiles[0],
        leaf_map[0].reshape(-1),
        mid_tiles[0],
        mid_map[0, 0],
        leaf_entries[0],
        mid_entries[0, 0],
        pivot,
    )
    received = lax.all_to_all(slots, "wide", split_axis=0, concat_axis=0, tiled=True)
    root_panel, block = pl.pallas_call(
        root_kernel,
        out_shape=[shape(rows_here, width), shape(BLOCK, BLOCK)],
        in_specs=[smem()] + [vmem()] * 5,
        out_specs=[vmem()] * 2,
        scratch_shapes=[
            pltpu.VMEM((PIVOT + rows_here, PIVOT), jnp.float32),
            pltpu.VMEM((BLOCK, PIVOT), jnp.float32),
            pltpu.VMEM((BLOCK, PIVOT), jnp.float32),
        ],
        compiler_params=pltpu.CompilerParams(vmem_limit_bytes=VMEM_BYTES),
        cost_estimate=pl.CostEstimate(flops=30_000_000_000, bytes_accessed=11_000_000, transcendentals=0),
        name="root",
    )(position, pivot, row_rows, column_rows, panel, root_update_entries[0, 0])
    noted = notes[:, 0, : UM + 1].astype(jnp.int32)
    targets, live = noted[:, :UM], noted[:, UM:]
    used = jnp.arange(UM, dtype=jnp.int32)[None, :] < live

    def place(block):
        return jnp.max(jnp.where(used & (targets // UR == block), targets - block * UR, -1), axis=1)

    row_place, column_place = place(position[0] // 8), place(position[0] % 8)
    spots = jnp.where(
        (row_place >= 0) & (column_place >= 0), row_place * UC + column_place, -1
    )
    total = pl.pallas_call(
        add_kernel,
        out_shape=shape(BLOCK, BLOCK),
        in_specs=[smem(), vmem(), vmem()],
        out_specs=vmem(),
        compiler_params=pltpu.CompilerParams(vmem_limit_bytes=VMEM_BYTES),
        name="add_tiles",
    )(spots, block, received)
    parts = pl.pallas_call(
        scatter_kernel,
        out_shape=shape(GROUPS, CHUNK, BLOCK),
        in_specs=[vmem()],
        out_specs=pl.BlockSpec(memory_space=pl.ANY),
        scratch_shapes=[pltpu.SemaphoreType.DMA((GROUPS,)), pltpu.SemaphoreType.DMA((GROUPS,))],
        compiler_params=pltpu.CompilerParams(collective_id=1, has_side_effects=True),
        name="scatter",
    )(total)
    top_part = pl.pallas_call(
        sum_kernel,
        out_shape=shape(CHUNK, BLOCK),
        in_specs=[vmem()],
        out_specs=vmem(),
        compiler_params=pltpu.CompilerParams(vmem_limit_bytes=VMEM_BYTES),
        name="sum_groups",
    )(parts)
    return (root_panel[None], top_part[None])


def solution(mesh):
    placed = (
        P("grp", "wide", None, None),
        P("grp", "wide"),
        P("grp", "wide", None),
        P("grp", "wide", None, None),
        P("grp", "wide"),
        P("grp", "wide", None),
        P("grp", "wide", None),
        P("grp", "wide", None, None),
    )
    return jax.shard_map(
        shards,
        mesh=mesh,
        in_specs=placed,
        out_specs=(P("grp", "wide", None), P("wide", "grp", None)),
        check_vma=False,
    )
```
